256 devices in a mesh: dp: 8 (over x, core), expert: 32 (over y, z).
Axes of the slice: x: 4, y: 4, z: 8, core: 2. Of those that a mesh axis runs over, the one named last changes fastest.
Arguments:
- tokens: bfloat16 [32768, 2048], P(('dp', 'expert')), may hold values from -6 to 6
- norm_gain: bfloat16 [2048], replicated, may hold values from 0.099609375 to 1.8984375
- router_weight: bfloat16 [2048, 32], replicated, may hold values from -0.1875 to 0.1875
- w_gate: bfloat16 [32, 2048, 5120], P('expert', None, 'dp'), may hold values from -0.125 to 0.125
- w_up: bfloat16 [32, 2048, 5120], P('expert', None, 'dp'), may hold values from -0.125 to 0.125
- w_down: bfloat16 [32, 5120, 2048], P('expert', 'dp'), may hold values from -0.078125 to 0.078125
- selected: int32 [32, 1792], replicated, may hold values from 0 to 32767, as said below
Outputs:
- combined: bfloat16 [32768, 2048], P(('dp', 'expert'))
The draws below stay inside these ranges and needn't reach their ends.
Inputs may be any that keep to these rules, and one draw needn't show every extreme that they name: `selected`: each row holds 1792 distinct token indices in ascending order. Of one row's indices at most 16 fall among one device's 128 tokens and at most 336 among the tokens of one index of dp; every row reaches both bounds.
All inputs are finite; a program needn't handle non-finite values.
Results may differ from the reference program's by a relative error of at most 0.0072.
Values may be sent and summed in bfloat16 or wider, within the bound.
A program may use at most 128 MiB of HBM per device.

```python
import jax
import jax.numpy as jnp
from jax import lax

D = 2048
FF = 5120
TOK_DEV = 128
EXPERTS = 32
TOKENS = 32768
CAP = 1792
PEAK = 16
RMOST = 336
N_DP = 8
N_EXPERT = 32


def choose_tokens(key):
    keys = jax.random.split(key, 7)
    row_cells = N_DP * RMOST
    row_score = jax.random.randint(keys[0], (N_DP, RMOST), 0, 1024) + 1024 * jax.random.randint(keys[1], (N_DP, 1), 0, 16)
    forced_row = jax.random.randint(keys[2], (), 0, N_DP)
    row_score = row_score + jnp.where(jnp.arange(N_DP) == forced_row, 32768, 0)[:, None]
    row_distinct = row_score.reshape(-1) * row_cells + jnp.arange(row_cells)
    row_order = jnp.argsort(-row_distinct)
    row_ranks = jnp.argsort(row_order)
    row_counts = jnp.sum((row_ranks < CAP).reshape(N_DP, RMOST).astype(jnp.int32), axis=1)
    source_cells = N_EXPERT * PEAK
    source_score = jax.random.randint(keys[3], (N_DP, N_EXPERT, PEAK), 0, 1024) + 1024 * jax.random.randint(keys[4], (N_DP, N_EXPERT, 1), 0, 16)
    forced_source = jax.random.randint(keys[5], (N_DP,), 0, N_EXPERT)
    source_score = source_score + jnp.where(jnp.arange(N_EXPERT)[None, :] == forced_source[:, None], 32768, 0)[:, :, None]
    source_distinct = source_score.reshape(N_DP, source_cells) * source_cells + jnp.arange(source_cells)[None, :]
    source_order = jnp.argsort(-source_distinct, axis=1)
    source_ranks = jnp.argsort(source_order, axis=1)
    chosen_cells = source_ranks < row_counts[:, None]
    source_counts = jnp.sum(chosen_cells.reshape(N_DP, N_EXPERT, PEAK).astype(jnp.int32), axis=2).reshape(-1)
    shuffled = jnp.argsort(jax.random.randint(keys[6], (N_DP * N_EXPERT, TOK_DEV), 0, 1073741824), axis=1)[:, :PEAK]
    candidates = jnp.arange(N_DP * N_EXPERT)[:, None] * TOK_DEV + shuffled
    usable = jnp.arange(PEAK)[None, :] < source_counts[:, None]
    sort_keys = jnp.where(usable, candidates, N_DP * N_EXPERT * TOK_DEV).reshape(-1)
    return jnp.sort(sort_keys)[:CAP].astype(jnp.int32)


def draw_selected(key, part):
    expert_keys = jax.random.split(jax.random.fold_in(key, 17), EXPERTS)
    return jax.vmap(choose_tokens)(expert_keys)


def levels(key, dims, cuts, low, largest):
    gain, own = 1.0, jax.random.fold_in(key, 6)
    for axis_at, blocks in cuts:
        draws = jnp.exp(jax.random.uniform(jax.random.fold_in(own, axis_at), (blocks,), jnp.float32, low / len(cuts), largest / len(cuts)))
        gain = gain * jnp.repeat(draws, dims[axis_at] // blocks).reshape([-1 if axis == axis_at else 1 for axis in range(len(dims))])
    return gain


def normal_values(own_key, dims, width, bound, shards=(), dtype=jnp.bfloat16):
    values = jax.random.normal(own_key, dims, jnp.float32) * width
    if len(shards) > 0:
        values = levels(own_key, dims, shards, -0.22, 0.18) * values
    return jnp.clip(values, min=-bound, max=bound).astype(dtype)


def setup_inputs(seed: int = 0) -> dict:
    seeds = jax.random.split(jax.random.key(seed), 8)
    tokens = normal_values(seeds[0], (TOKENS, D), 1.0, 6.0, ((0, 256),))
    norm_gain = jnp.clip(1.0 + 0.18 * jax.random.normal(seeds[1], (D,), jnp.float32), 0.099609375, 1.8984375).astype(jnp.bfloat16)
    router_weight = normal_values(seeds[2], (D, EXPERTS), (D // 2) ** -0.5, 0.1875)
    w_gate = normal_values(seeds[3], (EXPERTS, D, FF), D ** -0.5, 0.125, ((0, 32), (2, 8)))
    w_up = normal_values(seeds[4], (EXPERTS, D, FF), D ** -0.5, 0.125, ((0, 32), (2, 8)))
    w_down = normal_values(seeds[5], (EXPERTS, FF, D), FF ** -0.5, 0.078125, ((0, 32), (1, 8)))
    selected = draw_selected(jax.random.fold_in(seeds[7], 71), 0)
    return dict(tokens=tokens, norm_gain=norm_gain, router_weight=router_weight, w_gate=w_gate, w_up=w_up, w_down=w_down, selected=selected)


def reference(tokens, norm_gain, router_weight, w_gate, w_up, w_down, selected):
    activations = tokens.astype(jnp.float32)
    mean_square = lax.optimization_barrier(jnp.mean(activations * activations, axis=1, keepdims=True))
    normed = (activations * lax.rsqrt(mean_square + 1e-06) * norm_gain.astype(jnp.float32)).astype(jnp.bfloat16)
    gate_probs = jax.nn.sigmoid(jnp.dot(normed, router_weight, preferred_element_type=jnp.float32))
    probs_by_expert = gate_probs.T

    def per_expert(total, inputs):
        gate_matrix, up_matrix, down_matrix, chosen, probs = inputs
        expert_rows = normed[chosen]
        gate_part = jnp.dot(expert_rows, gate_matrix, preferred_element_type=jnp.float32)
        up_part = jnp.dot(expert_rows, up_matrix, preferred_element_type=jnp.float32)
        hidden = (jax.nn.gelu(gate_part, approximate=True) * up_part).astype(jnp.bfloat16)
        expert_out = jnp.dot(hidden, down_matrix, preferred_element_type=jnp.float32).astype(jnp.bfloat16)
        weights = probs[chosen]
        total = total.at[chosen].add(weights[:, None] * expert_out.astype(jnp.float32))
        return (total, None)
    start = jnp.zeros(normed.shape, jnp.float32)
    total, unused = lax.scan(per_expert, start, (w_gate, w_up, w_down, selected.astype(jnp.int32), probs_by_expert))
    return total.astype(jnp.bfloat16)
```

```python
import functools

import jax
import jax.numpy as jnp
from jax import lax
from jax.experimental import pallas as pl
from jax.experimental.pallas import tpu as pltpu
from jax.sharding import PartitionSpec as P

SLOT = 16
ROOM = 336
HALF = 176
CHUNKS = 8


def copy_pairs(mesh_id):
    return functools.partial(pltpu.make_async_remote_copy, device_id_type=mesh_id)


def moe_kernel(
    n_expert,
    s_ref,
    n_ref,
    p_ref,
    q_ref,
    mh_ref,
    ml_ref,
    wg_ref,
    wu_ref,
    wd_ref,
    o_ref,
    outg,
    recv,
    gath,
    acc,
    hid,
    wgu,
    wdn,
    prec,
    hrec,
    srec,
    arr,
    wsem,
    a_s,
    a_r,
    g_s,
    g_r,
    r_s,
    r_r,
    b_s,
    b_r,
):
    nc = CHUNKS
    width = outg.shape[2]
    ff = hid.shape[2]
    rows = n_expert * SLOT
    remote = copy_pairs(pl.DeviceIdType.MESH)
    d = lax.axis_index("dp")
    e = lax.axis_index("expert")
    x, core = d // 2, d % 2
    xr, xl, xo = (x + 1) % 4, (x + 3) % 4, (x + 2) % 4
    dl, dr, do, dq = xl * 2 + core, xr * 2 + core, xo * 2 + core, x * 2 + (1 - core)
    right, left, partner = (dr, e), (dl, e), (dq, e)

    def peer(k):
        return (d, (e + k) % n_expert)

    loads = [
        pltpu.make_async_copy(wg_ref, wgu.at[:, pl.ds(0, ff)], wsem.at[0]),
        pltpu.make_async_copy(wu_ref, wgu.at[:, pl.ds(ff, ff)], wsem.at[1]),
        pltpu.make_async_copy(wd_ref, wdn, wsem.at[2]),
    ]
    for load in loads:
        load.start()

    barrier = pltpu.get_barrier_semaphore()

    def greet(k, carry):
        pl.semaphore_signal(barrier, inc=1, device_id=peer(k), device_id_type=pl.DeviceIdType.MESH)
        return carry

    lax.fori_loop(1, n_expert, greet, 0)
    for who in (right, left, partner):
        pl.semaphore_signal(barrier, inc=1, device_id=who, device_id_type=pl.DeviceIdType.MESH)

    def lanes(c):
        return pl.ds(pl.multiple_of(c * width, width), width)

    def fill(c, carry):
        outg[c] = jnp.dot(
            s_ref[...], n_ref[:, lanes(c)], preferred_element_type=jnp.float32
        ).astype(jnp.bfloat16)
        return carry

    lax.fori_loop(0, nc, fill, 0)
    acc[...] = jnp.zeros_like(acc)
    pl.semaphore_wait(barrier, n_expert - 1 + 3)

    def slot(k):
        return pl.ds(pl.multiple_of(k * SLOT, SLOT), SLOT)

    def scatter(src, dst, send, got):
        def chunk(c, carry):
            def one(k, carry):
                to = (e + k) % n_expert
                remote(
                    src_ref=src.at[c, slot(to)],
                    dst_ref=dst.at[c, slot(e)],
                    send_sem=send.at[c],
                    recv_sem=got.at[c],
                    device_id=(d, to),
                ).start()
                return carry

            lax.fori_loop(1, n_expert, one, 0)
            pltpu.make_async_copy(src.at[c, slot(e)], dst.at[c, slot(e)], got.at[c]).start()
            return carry

        return chunk

    def all_got(dst, got, c):
        pltpu.make_async_copy(dst.at[c], dst.at[c], got.at[c]).wait()

    def all_sent(src, send, c):
        part = src.at[c, pl.ds(0, rows - SLOT)]
        pltpu.make_async_copy(part, part, send.at[c]).wait()

    lax.fori_loop(0, nc, scatter(outg, recv, a_s, a_r), 0)

    lo, hi = pl.ds(0, HALF), pl.ds(HALF, ROOM - HALF)

    def gcopy(c, j):
        block, to = [
            (gath.at[c, d], right),
            (gath.at[c, d], left),
            (gath.at[c, d], partner),
            (gath.at[c, dl, lo], right),
            (gath.at[c, dr, hi], left),
            (gath.at[c, dl], partner),
            (gath.at[c, dr], partner),
            (gath.at[c, do], partner),
        ][j]
        return remote(
            src_ref=block,
            dst_ref=block,
            send_sem=g_s.at[c, j],
            recv_sem=g_r.at[c, j],
            device_id=to,
        )

    def up(c, b):
        total = acc[b] + jnp.dot(
            gath[c, b],
            wgu[pl.ds(pl.multiple_of(c * width, width), width), :],
            preferred_element_type=jnp.float32,
        )

        @pl.when(c < nc - 1)
        def _():
            acc[b] = total

        @pl.when(c == nc - 1)
        def _():
            v, u = total[:, :ff], total[:, ff:]
            act = 0.5 * v * (1.0 + jnp.tanh(0.7978845608028654 * (v + 0.044715 * (v * v * v))))
            hid[b] = (act * u).astype(jnp.bfloat16)

    for load in loads:
        load.wait()

    def several(c, blocks):
        def step(i, carry):
            b = blocks[-1]
            for n in range(len(blocks) - 2, -1, -1):
                b = jnp.where(i == n, blocks[n], b)
            up(c, b)
            return carry

        lax.fori_loop(0, len(blocks), step, 0)

    def dispatch(i, carry):
        @pl.when(i < nc)
        def _():
            c = i
            all_got(recv, a_r, c)
            gath[c, d] = jnp.dot(
                p_ref[...], recv[c], preferred_element_type=jnp.float32
            ).astype(jnp.bfloat16)
            for j in (0, 1, 2):
                gcopy(c, j).start()

        @pl.when((i >= 1) & (i < nc + 1))
        def _():
            c = i - 1
            gcopy(c, 0).wait_recv()
            gcopy(c, 3).start()
            gcopy(c, 1).wait_recv()
            gcopy(c, 4).start()
            gcopy(c, 5).start()
            gcopy(c, 6).start()
            gcopy(c, 2).wait_recv()
            several(c, (d, dl, dr, dq))

        @pl.when((i >= 2) & (i < nc + 2))
        def _():
            c = i - 2
            gcopy(c, 3).wait_recv()
            gcopy(c, 4).wait_recv()
            gcopy(c, 7).start()
            gcopy(c, 5).wait_recv()
            gcopy(c, 6).wait_recv()
            several(c, (do, xl * 2 + (1 - core), xr * 2 + (1 - core)))
            gcopy(c, 7).wait_recv()
            several(c, (xo * 2 + (1 - core),))

        return carry

    lax.fori_loop(0, nc + 2, dispatch, 0)

    def drain(c, carry):
        for j in range(8):
            gcopy(c, j).wait_send()
        all_sent(outg, a_s, c)
        return carry

    lax.fori_loop(0, nc, drain, 0)

    def mine(c, k):
        return acc.at[k + 4 * (c % 2), :, pl.ds(pl.multiple_of((c // 2) * width, width), width)]

    def rcopy(c, j):
        src, dst, to = [
            (gath.at[c, 0], prec.at[c, 0], partner),
            (gath.at[c, 1], prec.at[c, 1], partner),
            (gath.at[c, 2], prec.at[c, 2], partner),
            (gath.at[c, 3], prec.at[c, 3], partner),
            (gath.at[c, 4, lo], hrec.at[c, lo], right),
            (gath.at[c, 4, hi], hrec.at[c, hi], left),
            (gath.at[c, 5], srec.at[c, 0], right),
            (gath.at[c, 6], srec.at[c, 1], left),
        ][j]
        return remote(
            src_ref=src, dst_ref=dst, send_sem=r_s.at[c, j], recv_sem=r_r.at[c, j], device_id=to
        )

    def down(c, b):
        return jnp.dot(hid[b], wdn[:, lanes(c)], preferred_element_type=jnp.float32)

    def pair(c, k):
        return mine(c, k)[...] + prec[c, k].astype(jnp.float32)

    def combine(i, carry):
        @pl.when(i < nc)
        def _():
            c = i

            for k in range(4):
                gath[c, k] = down(c, k * 2 + (1 - core)).astype(jnp.bfloat16)
                rcopy(c, k).start()

            def keep(k, carry):
                mine(c, k)[...] = down(c, k * 2 + core)
                return carry

            lax.fori_loop(0, 4, keep, 0)

        @pl.when((i >= 1) & (i < nc + 1))
        def _():
            c = i - 1
            for k in range(4):
                rcopy(c, k).wait_recv()
            gath[c, 4] = pair(c, xo).astype(jnp.bfloat16)
            rcopy(c, 4).start()
            rcopy(c, 5).start()

        @pl.when((i >= 2) & (i < nc + 2))
        def _():
            c = i - 2
            to_right, to_left = pair(c, xr), pair(c, xl)
            rcopy(c, 4).wait_recv()
            gath[c, 5, lo] = (to_right[:HALF] + hrec[c, lo].astype(jnp.float32)).astype(jnp.bfloat16)
            gath[c, 5, hi] = to_right[HALF:].astype(jnp.bfloat16)
            rcopy(c, 6).start()
            rcopy(c, 5).wait_recv()
            gath[c, 6, lo] = to_left[:HALF].astype(jnp.bfloat16)
            gath[c, 6, hi] = (to_left[HALF:] + hrec[c, hi].astype(jnp.float32)).astype(jnp.bfloat16)
            rcopy(c, 7).start()

        @pl.when(i >= 3)
        def _():
            c = i - 3
            total = pair(c, x)
            rcopy(c, 6).wait_recv()
            rcopy(c, 7).wait_recv()
            total = total + srec[c, 0].astype(jnp.float32) + srec[c, 1].astype(jnp.float32)
            outg[c] = jnp.dot(
                q_ref[...], total.astype(jnp.bfloat16), preferred_element_type=jnp.float32
            ).astype(jnp.bfloat16)
            scatter(outg, arr, b_s, b_r)(c, 0)

        return carry

    lax.fori_loop(0, nc + 3, combine, 0)

    def finish(c, carry):
        all_got(arr, b_r, c)
        got = arr[c]
        o_ref[:, lanes(c)] = (
            jnp.dot(mh_ref[...], got, preferred_element_type=jnp.float32)
            + jnp.dot(ml_ref[...], got, preferred_element_type=jnp.float32)
        ).astype(jnp.bfloat16)
        return carry

    lax.fori_loop(0, nc, finish, 0)

    def drain_back(c, carry):
        for j in range(8):
            rcopy(c, j).wait_send()
        all_sent(outg, b_s, c)
        return carry

    lax.fori_loop(0, nc, drain_back, 0)


def per_device(tokens, norm_gain, router_weight, w_gate, w_up, w_down, selected):
    n_dp = lax.axis_size("dp")
    n_expert = lax.axis_size("expert")
    tok_rows, model_width = tokens.shape
    experts, capacity = selected.shape
    ff = w_gate.shape[2]
    width = model_width // CHUNKS
    rows = n_expert * SLOT
    d = lax.axis_index("dp")
    e = lax.axis_index("expert")
    activations = tokens.astype(jnp.float32)
    mean_square = jnp.mean(activations * activations, axis=1, keepdims=True)
    normed = (activations * lax.rsqrt(mean_square + 1e-06) * norm_gain.astype(jnp.float32)).astype(
        jnp.bfloat16
    )
    gate_probs = jax.nn.sigmoid(jnp.dot(normed, router_weight, preferred_element_type=jnp.float32))

    lowest = (d * n_expert + e) * tok_rows
    below = jnp.sum((selected < lowest).astype(jnp.int32), axis=1, keepdims=True)
    inside = (selected >= lowest) & (selected < lowest + tok_rows)
    rank = jnp.arange(capacity, dtype=jnp.int32)[None, :] - below
    slots = jnp.arange(SLOT, dtype=jnp.int32)
    local = jnp.sum(
        jnp.where(
            inside[:, None, :] & (rank[:, None, :] == slots[None, :, None]),
            selected[:, None, :] - lowest + 1,
            0,
        ),
        axis=2,
    )
    token_range = jnp.arange(1, tok_rows + 1, dtype=jnp.int32)
    flat = local.reshape(rows)
    take = (flat[:, None] == token_range[None, :]).astype(jnp.bfloat16)
    mix = jnp.where(
        token_range[:, None, None] == local[None, :, :], gate_probs[:, :, None], 0.0
    ).reshape(tok_rows, rows)
    mix_high = lax.reduce_precision(mix, 8, 7)
    mix_low = (mix - mix_high).astype(jnp.bfloat16)
    mix_high = mix_high.astype(jnp.bfloat16)

    expert_row = lax.dynamic_index_in_dim(selected, e, 0, keepdims=False)
    bounds = (d * n_expert + jnp.arange(n_expert + 1, dtype=jnp.int32)) * tok_rows
    counts = jnp.sum((expert_row[None, :] < bounds[:, None]).astype(jnp.int32), axis=1)
    first, last = counts[:-1], counts[1:]
    place = first[:, None] - counts[0] + slots[None, :]
    place = jnp.where(slots[None, :] < (last - first)[:, None], place, -1).reshape(rows)
    room = jnp.arange(ROOM, dtype=jnp.int32)
    pack = (room[:, None] == place[None, :]).astype(jnp.bfloat16)
    unpack = (place[:, None] == room[None, :]).astype(jnp.bfloat16)

    vmem = pl.BlockSpec(memory_space=pltpu.VMEM)
    hbm = pl.BlockSpec(memory_space=pl.ANY)
    bf16, f32 = jnp.bfloat16, jnp.float32
    dma = pltpu.SemaphoreType.DMA
    return pl.pallas_call(
        functools.partial(moe_kernel, n_expert),
        out_shape=jax.ShapeDtypeStruct((tok_rows, model_width), bf16),
        in_specs=[vmem] * 6 + [hbm] * 3,
        out_specs=vmem,
        scratch_shapes=[
            pltpu.VMEM((CHUNKS, rows, width), bf16),
            pltpu.VMEM((CHUNKS, rows, width), bf16),
            pltpu.VMEM((CHUNKS, n_dp, ROOM, width), bf16),
            pltpu.VMEM((n_dp, ROOM, 2 * ff), f32),
            pltpu.VMEM((n_dp, ROOM, ff), bf16),
            pltpu.VMEM((model_width, 2 * ff), bf16),
            pltpu.VMEM((ff, model_width), bf16),
            pltpu.VMEM((CHUNKS, n_dp // 2, ROOM, width), bf16),
            pltpu.VMEM((CHUNKS, ROOM, width), bf16),
            pltpu.VMEM((CHUNKS, 2, ROOM, width), bf16),
            pltpu.VMEM((CHUNKS, rows, width), bf16),
            dma((3,)),
            dma((CHUNKS,)),
            dma((CHUNKS,)),
            dma((CHUNKS, 8)),
            dma((CHUNKS, 8)),
            dma((CHUNKS, 8)),
            dma((CHUNKS, 8)),
            dma((CHUNKS,)),
            dma((CHUNKS,)),
        ],
        compiler_params=pltpu.CompilerParams(
            collective_id=0, has_side_effects=True, vmem_limit_bytes=67043328
        ),
    )(
        take,
        normed,
        pack,
        unpack,
        mix_high,
        mix_low,
        w_gate.reshape(model_width, ff),
        w_up.reshape(model_width, ff),
        w_down.reshape(ff, model_width),
    )


def solution(mesh):
    in_specs = (
        P(("dp", "expert"), None),
        P(),
        P(),
        P("expert", None, "dp"),
        P("expert", None, "dp"),
        P("expert", "dp", None),
        P(),
    )
    out_specs = P(("dp", "expert"), None)
    return jax.shard_map(
        per_device, mesh=mesh, in_specs=in_specs, out_specs=out_specs, check_vma=False
    )
```

```python
import functools

import jax
import jax.numpy as jnp
from jax import lax
from jax.experimental import pallas as pl
from jax.experimental.pallas import tpu as pltpu
from jax.sharding import PartitionSpec as P

SLOT = 16
ROOM = 336
HALF = 176
CHUNKS = 8


def copy_pairs(mesh_id):
    return functools.partial(pltpu.make_async_remote_copy, device_id_type=mesh_id)


def moe_kernel(
    n_expert,
    tok_ref,
    gain_ref,
    rw_ref,
    sel_ref,
    wg_ref,
    wu_ref,
    wd_ref,
    o_ref,
    outg,
    recv,
    gath,
    acc,
    hid,
    wgu,
    wdn,
    prec,
    hrec,
    srec,
    arr,
    s_ref,
    n_ref,
    p_ref,
    q_ref,
    m_ref,
    lg_ref,
    gt_ref,
    wsem,
    a_s,
    a_r,
    g_s,
    g_r,
    r_s,
    r_r,
    b_s,
    b_r,
):
    nc = CHUNKS
    width = outg.shape[2]
    ff = hid.shape[2]
    rows = n_expert * SLOT
    remote = copy_pairs(pl.DeviceIdType.MESH)
    d = lax.axis_index("dp")
    e = lax.axis_index("expert")
    x, core = d // 2, d % 2
    xr, xl, xo = (x + 1) % 4, (x + 3) % 4, (x + 2) % 4
    dl, dr, do, dq = xl * 2 + core, xr * 2 + core, xo * 2 + core, x * 2 + (1 - core)
    right, left, partner = (dr, e), (dl, e), (dq, e)

    def peer(k):
        return (d, (e + k) % n_expert)

    barrier = pltpu.get_barrier_semaphore()

    def greet(k, carry):
        pl.semaphore_signal(barrier, inc=1, device_id=peer(k), device_id_type=pl.DeviceIdType.MESH)
        return carry

    lax.fori_loop(1, n_expert, greet, 0)
    for who in (right, left, partner):
        pl.semaphore_signal(barrier, inc=1, device_id=who, device_id_type=pl.DeviceIdType.MESH)

    def lanes(c):
        return pl.ds(pl.multiple_of(c * width, width), width)

    loads = [
        pltpu.make_async_copy(wg_ref, wgu.at[:, pl.ds(0, ff)], wsem.at[0]),
        pltpu.make_async_copy(wu_ref, wgu.at[:, pl.ds(ff, ff)], wsem.at[1]),
        pltpu.make_async_copy(wd_ref, wdn, wsem.at[2]),
    ]
    for load in loads:
        load.start()

    f32, bf16 = jnp.float32, jnp.bfloat16
    tok_rows = tok_ref.shape[0]
    experts, capacity = sel_ref.shape

    def iota(shape, axis):
        return lax.broadcasted_iota(jnp.int32, shape, axis)

    def one_hot(mask):
        return jnp.where(mask, 1.0, 0.0).astype(bf16)

    def flip(a):
        n = a.shape[1]
        eye = one_hot(iota((n, n), 0) == iota((n, n), 1))
        turned = lax.dot_general(eye, a, (((1,), (1,)), ((), ())), preferred_element_type=f32)
        return turned.astype(bf16)

    tok = tok_ref[...].astype(f32)
    mean_square = jnp.mean(tok * tok, axis=1, keepdims=True)
    n_ref[...] = (tok * lax.rsqrt(mean_square + 1e-06) * gain_ref[...].astype(f32)).astype(bf16)

    lowest = (d * n_expert + e) * tok_rows
    sel = sel_ref[...]
    below = jnp.sum(jnp.where(sel < lowest, 1.0, 0.0), axis=1, keepdims=True)
    rank = iota((experts, capacity), 1).astype(f32) - below
    inside = (sel >= lowest) & (sel < lowest + tok_rows)
    local = jnp.where(inside, sel - lowest + 1, 0).astype(f32)
    token = iota((experts, tok_rows), 1).astype(f32) + 1.0
    by_slot = []
    for k in range(SLOT):
        found = jnp.sum(jnp.where(rank == float(k), local, 0.0), axis=1, keepdims=True)
        by_slot.append(jnp.where(found == token, 1.0, 0.0))
    by_slot = jnp.concatenate(by_slot, axis=0).astype(bf16)
    r = iota((rows, rows), 0)
    order = one_hot(iota((rows, rows), 1) == (r & (SLOT - 1)) * experts + lax.shift_right_logical(r, 4))
    s_ref[...] = jnp.dot(order, by_slot, preferred_element_type=f32).astype(bf16)
    pl.semaphore_wait(barrier, n_expert - 1 + 3)

    def slot(k):
        return pl.ds(pl.multiple_of(k * SLOT, SLOT), SLOT)

    def scatter(src, dst, send, got):
        def chunk(c, carry):
            def one(k, carry):
                to = (e + k) % n_expert
                remote(
                    src_ref=src.at[c, slot(to)],
                    dst_ref=dst.at[c, slot(e)],
                    send_sem=send.at[c],
                    recv_sem=got.at[c],
                    device_id=(d, to),
                ).start()
                return carry

            lax.fori_loop(1, n_expert, one, 0)
            pltpu.make_async_copy(src.at[c, slot(e)], dst.at[c, slot(e)], got.at[c]).start()
            return carry

        return chunk

    def all_got(dst, got, c):
        pltpu.make_async_copy(dst.at[c], dst.at[c], got.at[c]).wait()

    def all_sent(src, send, c):
        part = src.at[c, pl.ds(0, rows - SLOT)]
        pltpu.make_async_copy(part, part, send.at[c]).wait()

    def fill(c, carry):
        outg[c] = jnp.dot(s_ref[...], n_ref[:, lanes(c)], preferred_element_type=f32).astype(bf16)
        return scatter(outg, recv, a_s, a_r)(c, carry)

    lax.fori_loop(0, nc, fill, 0)

    row = sel_ref[pl.ds(e, 1), :]
    slot_row = iota((rows, 1), 0)
    lower = (d * n_expert + lax.shift_right_logical(slot_row, 4)) * tok_rows
    rank_in = (slot_row & (SLOT - 1)).astype(f32)
    first = jnp.sum(jnp.where(row < lower, 1.0, 0.0), axis=1, keepdims=True)
    last = jnp.sum(jnp.where(row < lower + tok_rows, 1.0, 0.0), axis=1, keepdims=True)
    start = jnp.sum(jnp.where(row < d * (n_expert * tok_rows), 1.0, 0.0), axis=1, keepdims=True)
    place = jnp.where(rank_in < last - first, first - start + rank_in, -1.0)
    q_ref[...] = one_hot(place == iota((rows, ROOM), 1).astype(f32))
    p_ref[...] = flip(q_ref[...])
    m_ref[...] = flip(s_ref[...])
    acc[...] = jnp.zeros_like(acc)
    lg_ref[...] = jnp.zeros_like(lg_ref)

    lo, hi = pl.ds(0, HALF), pl.ds(HALF, ROOM - HALF)

    def gcopy(c, j):
        block, to = [
            (gath.at[c, d], right),
            (gath.at[c, d], left),
            (gath.at[c, d], partner),
            (gath.at[c, dl, lo], right),
            (gath.at[c, dr, hi], left),
            (gath.at[c, dl], partner),
            (gath.at[c, dr], partner),
            (gath.at[c, do], partner),
        ][j]
        return remote(
            src_ref=block,
            dst_ref=block,
            send_sem=g_s.at[c, j],
            recv_sem=g_r.at[c, j],
            device_id=to,
        )

    def up(c, b):
        total = acc[b] + jnp.dot(
            gath[c, b],
            wgu[pl.ds(pl.multiple_of(c * width, width), width), :],
            preferred_element_type=jnp.float32,
        )

        @pl.when(c < nc - 1)
        def _():
            acc[b] = total

        @pl.when(c == nc - 1)
        def _():
            v, u = total[:, :ff], total[:, ff:]
            act = 0.5 * v * (1.0 + jnp.tanh(0.7978845608028654 * (v + 0.044715 * (v * v * v))))
            hid[b] = (act * u).astype(jnp.bfloat16)

    for load in loads:
        load.wait()

    def several(c, blocks):
        def step(i, carry):
            b = blocks[-1]
            for n in range(len(blocks) - 2, -1, -1):
                b = jnp.where(i == n, blocks[n], b)
            up(c, b)
            return carry

        lax.fori_loop(0, len(blocks), step, 0)

    def dispatch(i, carry):
        @pl.when(i < nc)
        def _():
            c = i
            all_got(recv, a_r, c)
            packed = jnp.dot(p_ref[...], recv[c], preferred_element_type=f32).astype(bf16)
            gath[c, d] = packed
            for j in (0, 1, 2):
                gcopy(c, j).start()
            lg_ref[...] += jnp.dot(
                packed,
                rw_ref[pl.ds(pl.multiple_of(c * width, width), width), :],
                preferred_element_type=f32,
            )

        @pl.when((i >= 1) & (i < nc + 1))
        def _():
            c = i - 1
            gcopy(c, 0).wait_recv()
            gcopy(c, 3).start()
            gcopy(c, 1).wait_recv()
            gcopy(c, 4).start()
            gcopy(c, 5).start()
            gcopy(c, 6).start()
            gcopy(c, 2).wait_recv()
            several(c, (d, dl, dr, dq))

        @pl.when((i >= 2) & (i < nc + 2))
        def _():
            c = i - 2
            gcopy(c, 3).wait_recv()
            gcopy(c, 4).wait_recv()
            gcopy(c, 7).start()
            gcopy(c, 5).wait_recv()
            gcopy(c, 6).wait_recv()
            several(c, (do, xl * 2 + (1 - core), xr * 2 + (1 - core)))
            gcopy(c, 7).wait_recv()
            several(c, (xo * 2 + (1 - core),))

        return carry

    lax.fori_loop(0, nc + 2, dispatch, 0)

    def drain(c, carry):
        for j in range(8):
            gcopy(c, j).wait_send()
        all_sent(outg, a_s, c)
        return carry

    lax.fori_loop(0, nc, drain, 0)

    own_logit = jnp.where(iota((ROOM, experts), 1) == e, lg_ref[...], 0.0)
    gate = jax.nn.sigmoid(jnp.sum(own_logit, axis=1, keepdims=True))
    gt_ref[...] = jnp.broadcast_to(gate, gt_ref.shape)

    def mine(c, k):
        return acc.at[k + 4 * (c % 2), :, pl.ds(pl.multiple_of((c // 2) * width, width), width)]

    def rcopy(c, j):
        src, dst, to = [
            (gath.at[c, 0], prec.at[c, 0], partner),
            (gath.at[c, 1], prec.at[c, 1], partner),
            (gath.at[c, 2], prec.at[c, 2], partner),
            (gath.at[c, 3], prec.at[c, 3], partner),
            (gath.at[c, 4, lo], hrec.at[c, lo], right),
            (gath.at[c, 4, hi], hrec.at[c, hi], left),
            (gath.at[c, 5], srec.at[c, 0], right),
            (gath.at[c, 6], srec.at[c, 1], left),
        ][j]
        return remote(
            src_ref=src, dst_ref=dst, send_sem=r_s.at[c, j], recv_sem=r_r.at[c, j], device_id=to
        )

    def down(c, b):
        return jnp.dot(hid[b], wdn[:, lanes(c)], preferred_element_type=jnp.float32)

    def pair(c, k):
        return mine(c, k)[...] + prec[c, k].astype(jnp.float32)

    def combine(i, carry):
        @pl.when(i < nc)
        def _():
            c = i

            for k in range(4):
                gath[c, k] = down(c, k * 2 + (1 - core)).astype(jnp.bfloat16)
                rcopy(c, k).start()

            def keep(k, carry):
                mine(c, k)[...] = down(c, k * 2 + core)
                return carry

            lax.fori_loop(0, 4, keep, 0)

        @pl.when((i >= 1) & (i < nc + 1))
        def _():
            c = i - 1
            for k in range(4):
                rcopy(c, k).wait_recv()
            gath[c, 4] = pair(c, xo).astype(jnp.bfloat16)
            rcopy(c, 4).start()
            rcopy(c, 5).start()

        @pl.when((i >= 2) & (i < nc + 2))
        def _():
            c = i - 2
            to_right, to_left = pair(c, xr), pair(c, xl)
            rcopy(c, 4).wait_recv()
            gath[c, 5, lo] = (to_right[:HALF] + hrec[c, lo].astype(jnp.float32)).astype(jnp.bfloat16)
            gath[c, 5, hi] = to_right[HALF:].astype(jnp.bfloat16)
            rcopy(c, 6).start()
            rcopy(c, 5).wait_recv()
            gath[c, 6, lo] = to_left[:HALF].astype(jnp.bfloat16)
            gath[c, 6, hi] = (to_left[HALF:] + hrec[c, hi].astype(jnp.float32)).astype(jnp.bfloat16)
            rcopy(c, 7).start()

        @pl.when(i >= 3)
        def _():
            c = i - 3
            total = pair(c, x)
            rcopy(c, 6).wait_recv()
            rcopy(c, 7).wait_recv()
            total = total + srec[c, 0].astype(jnp.float32) + srec[c, 1].astype(jnp.float32)
            total = total * gt_ref[...]
            outg[c] = jnp.dot(
                q_ref[...], total.astype(jnp.bfloat16), preferred_element_type=jnp.float32
            ).astype(jnp.bfloat16)
            scatter(outg, arr, b_s, b_r)(c, 0)

        return carry

    lax.fori_loop(0, nc + 3, combine, 0)

    def finish(c, carry):
        all_got(arr, b_r, c)
        got = arr[c]
        o_ref[:, lanes(c)] = jnp.dot(m_ref[...], got, preferred_element_type=f32).astype(bf16)
        return carry

    lax.fori_loop(0, nc, finish, 0)

    def drain_back(c, carry):
        for j in range(8):
            rcopy(c, j).wait_send()
        all_sent(outg, b_s, c)
        return carry

    lax.fori_loop(0, nc, drain_back, 0)


def per_device(tokens, norm_gain, router_weight, w_gate, w_up, w_down, selected):
    n_dp = lax.axis_size("dp")
    n_expert = lax.axis_size("expert")
    tok_rows, model_width = tokens.shape
    experts, capacity = selected.shape
    ff = w_gate.shape[2]
    width = model_width // CHUNKS
    rows = n_expert * SLOT
    vmem = pl.BlockSpec(memory_space=pltpu.VMEM)
    hbm = pl.BlockSpec(memory_space=pl.ANY)
    bf16, f32 = jnp.bfloat16, jnp.float32
    dma = pltpu.SemaphoreType.DMA
    return pl.pallas_call(
        functools.partial(moe_kernel, n_expert),
        out_shape=jax.ShapeDtypeStruct((tok_rows, model_width), bf16),
        in_specs=[vmem] * 4 + [hbm] * 3,
        out_specs=vmem,
        scratch_shapes=[
            pltpu.VMEM((CHUNKS, rows, width), bf16),
            pltpu.VMEM((CHUNKS, rows, width), bf16),
            pltpu.VMEM((CHUNKS, n_dp, ROOM, width), bf16),
            pltpu.VMEM((n_dp, ROOM, 2 * ff), f32),
            pltpu.VMEM((n_dp, ROOM, ff), bf16),
            pltpu.VMEM((model_width, 2 * ff), bf16),
            pltpu.VMEM((ff, model_width), bf16),
            pltpu.VMEM((CHUNKS, n_dp // 2, ROOM, width), bf16),
            pltpu.VMEM((CHUNKS, ROOM, width), bf16),
            pltpu.VMEM((CHUNKS, 2, ROOM, width), bf16),
            pltpu.VMEM((CHUNKS, rows, width), bf16),
            pltpu.VMEM((rows, tok_rows), bf16),
            pltpu.VMEM((tok_rows, model_width), bf16),
            pltpu.VMEM((ROOM, rows), bf16),
            pltpu.VMEM((rows, ROOM), bf16),
            pltpu.VMEM((tok_rows, rows), bf16),
            pltpu.VMEM((ROOM, experts), f32),
            pltpu.VMEM((ROOM, width), f32),
            dma((3,)),
            dma((CHUNKS,)),
            dma((CHUNKS,)),
            dma((CHUNKS, 8)),
            dma((CHUNKS, 8)),
            dma((CHUNKS, 8)),
            dma((CHUNKS, 8)),
            dma((CHUNKS,)),
            dma((CHUNKS,)),
        ],
        compiler_params=pltpu.CompilerParams(
            collective_id=0, has_side_effects=True, vmem_limit_bytes=67043328
        ),
    )(
        tokens,
        norm_gain.reshape(1, model_width),
        router_weight,
        selected,
        w_gate.reshape(model_width, ff),
        w_up.reshape(model_width, ff),
        w_down.reshape(ff, model_width),
    )


def solution(mesh):
    in_specs = (
        P(("dp", "expert"), None),
        P(),
        P(),
        P("expert", None, "dp"),
        P("expert", None, "dp"),
        P("expert", "dp", None),
        P(),
    )
    out_specs = P(("dp", "expert"), None)
    return jax.shard_map(
        per_device, mesh=mesh, in_specs=in_specs, out_specs=out_specs, check_vma=False
    )
```

```python
import functools

import jax
import jax.numpy as jnp
from jax import lax
from jax.experimental import pallas as pl
from jax.experimental.pallas import tpu as pltpu
from jax.sharding import PartitionSpec as P

SLOT = 16
ROOM = 336
HALF = 176
CHUNKS = 8


def copy_pairs(mesh_id):
    return functools.partial(pltpu.make_async_remote_copy, device_id_type=mesh_id)


def moe_kernel(
    n_expert,
    tok_ref,
    gain_ref,
    rw_ref,
    sel_ref,
    wg_ref,
    wu_ref,
    wd_ref,
    o_ref,
    outg,
    recv,
    gath,
    acc,
    hid,
    wgu,
    wdn,
    prec,
    hrec,
    srec,
    arr,
    s_ref,
    n_ref,
    p_ref,
    q_ref,
    m_ref,
    lg_ref,
    gt_ref,
    wsem,
    a_s,
    a_r,
    g_s,
    g_r,
    r_s,
    r_r,
    b_s,
    b_r,
):
    nc = CHUNKS
    width = outg.shape[2]
    ff = hid.shape[2]
    rows = n_expert * SLOT
    remote = copy_pairs(pl.DeviceIdType.MESH)
    d = lax.axis_index("dp")
    e = lax.axis_index("expert")
    x, core = d // 2, d % 2
    xr, xl, xo = (x + 1) % 4, (x + 3) % 4, (x + 2) % 4
    dl, dr, do, dq = xl * 2 + core, xr * 2 + core, xo * 2 + core, x * 2 + (1 - core)
    right, left, partner = (dr, e), (dl, e), (dq, e)

    def peer(k):
        return (d, (e + k) % n_expert)

    barrier = pltpu.get_barrier_semaphore()

    def greet(k, carry):
        pl.semaphore_signal(barrier, inc=1, device_id=peer(k), device_id_type=pl.DeviceIdType.MESH)
        return carry

    lax.fori_loop(1, n_expert, greet, 0)
    for who in (right, left, partner):
        pl.semaphore_signal(barrier, inc=1, device_id=who, device_id_type=pl.DeviceIdType.MESH)

    def lanes(c):
        return pl.ds(pl.multiple_of(c * width, width), width)

    loads = [
        pltpu.make_async_copy(wg_ref, wgu.at[:, pl.ds(0, ff)], wsem.at[0]),
        pltpu.make_async_copy(wu_ref, wgu.at[:, pl.ds(ff, ff)], wsem.at[1]),
        pltpu.make_async_copy(wd_ref, wdn, wsem.at[2]),
    ]
    for load in loads:
        load.start()

    f32, bf16 = jnp.float32, jnp.bfloat16
    tok_rows = tok_ref.shape[0]
    experts, capacity = sel_ref.shape

    def iota(shape, axis):
        return lax.broadcasted_iota(jnp.int32, shape, axis)

    def one_hot(mask):
        return jnp.where(mask, 1.0, 0.0).astype(bf16)

    def flip(a):
        n = a.shape[1]
        eye = one_hot(iota((n, n), 0) == iota((n, n), 1))
        turned = lax.dot_general(eye, a, (((1,), (1,)), ((), ())), preferred_element_type=f32)
        return turned.astype(bf16)

    tok = tok_ref[...].astype(f32)
    mean_square = jnp.mean(tok * tok, axis=1, keepdims=True)
    n_ref[...] = (tok * lax.rsqrt(mean_square + 1e-06) * gain_ref[...].astype(f32)[None, :]).astype(bf16)

    lowest = (d * n_expert + e) * tok_rows
    sel = sel_ref[...]
    below = jnp.sum(jnp.where(sel < lowest, 1.0, 0.0), axis=1, keepdims=True)
    rank = iota((experts, capacity), 1).astype(f32) - below
    inside = (sel >= lowest) & (sel < lowest + tok_rows)
    local = jnp.where(inside, sel - lowest + 1, 0).astype(f32)
    token = iota((experts, tok_rows), 1).astype(f32) + 1.0
    by_slot = []
    for k in range(SLOT):
        found = jnp.sum(jnp.where(rank == float(k), local, 0.0), axis=1, keepdims=True)
        by_slot.append(jnp.where(found == token, 1.0, 0.0))
    by_slot = jnp.concatenate(by_slot, axis=0).astype(bf16)
    r = iota((rows, rows), 0)
    order = one_hot(iota((rows, rows), 1) == (r & (SLOT - 1)) * experts + lax.shift_right_logical(r, 4))
    s_ref[...] = jnp.dot(order, by_slot, preferred_element_type=f32).astype(bf16)
    pl.semaphore_wait(barrier, n_expert - 1 + 3)

    def slot(k):
        return pl.ds(pl.multiple_of(k * SLOT, SLOT), SLOT)

    def scatter(src, dst, send, got):
        def chunk(c, carry):
            def one(k, carry):
                to = (e + k) % n_expert
                remote(
                    src_ref=src.at[c, slot(to)],
                    dst_ref=dst.at[c, slot(e)],
                    send_sem=send.at[c],
                    recv_sem=got.at[c],
                    device_id=(d, to),
                ).start()
                return carry

            lax.fori_loop(1, n_expert, one, 0)
            pltpu.make_async_copy(src.at[c, slot(e)], dst.at[c, slot(e)], got.at[c]).start()
            return carry

        return chunk

    def all_got(dst, got, c):
        pltpu.make_async_copy(dst.at[c], dst.at[c], got.at[c]).wait()

    def all_sent(src, send, c):
        part = src.at[c, pl.ds(0, rows - SLOT)]
        pltpu.make_async_copy(part, part, send.at[c]).wait()

    def fill(c, carry):
        outg[c] = jnp.dot(s_ref[...], n_ref[:, lanes(c)], preferred_element_type=f32).astype(bf16)
        return scatter(outg, recv, a_s, a_r)(c, carry)

    lax.fori_loop(0, nc, fill, 0)

    row = sel_ref[pl.ds(e, 1), :]
    slot_row = iota((rows, 1), 0)
    lower = (d * n_expert + lax.shift_right_logical(slot_row, 4)) * tok_rows
    rank_in = (slot_row & (SLOT - 1)).astype(f32)
    first = jnp.sum(jnp.where(row < lower, 1.0, 0.0), axis=1, keepdims=True)
    last = jnp.sum(jnp.where(row < lower + tok_rows, 1.0, 0.0), axis=1, keepdims=True)
    start = jnp.sum(jnp.where(row < d * (n_expert * tok_rows), 1.0, 0.0), axis=1, keepdims=True)
    place = jnp.where(rank_in < last - first, first - start + rank_in, -1.0)
    q_ref[...] = one_hot(place == iota((rows, ROOM), 1).astype(f32))
    p_ref[...] = flip(q_ref[...])
    m_ref[...] = flip(s_ref[...])
    acc[...] = jnp.zeros_like(acc)
    lg_ref[...] = jnp.zeros_like(lg_ref)

    lo, hi = pl.ds(0, HALF), pl.ds(HALF, ROOM - HALF)

    def gcopy(c, j):
        block, to = [
            (gath.at[c, d], right),
            (gath.at[c, d], left),
            (gath.at[c, d], partner),
            (gath.at[c, dl, lo], right),
            (gath.at[c, dr, hi], left),
            (gath.at[c, dl], partner),
            (gath.at[c, dr], partner),
            (gath.at[c, do], partner),
        ][j]
        return remote(
            src_ref=block,
            dst_ref=block,
            send_sem=g_s.at[c, j],
            recv_sem=g_r.at[c, j],
            device_id=to,
        )

    def act(v, u):
        g = 0.5 * v * (1.0 + jnp.tanh(0.7978845608028654 * (v + 0.044715 * (v * v * v))))
        return (g * u).astype(bf16)

    def up(c, b):
        @pl.when((c % 2 == 1) & (c < nc - 1))
        def _():
            a = jnp.concatenate([gath[c - 1, b], gath[c, b]], axis=1)
            w = pl.ds(pl.multiple_of((c - 1) * width, 2 * width), 2 * width)
            acc[b] += jnp.dot(a, wgu[w, :], preferred_element_type=f32)

        @pl.when(c == nc - 1)
        def _():
            a = jnp.concatenate([gath[c - 1, b], gath[c, b]], axis=1)
            w = pl.ds(pl.multiple_of((c - 1) * width, 2 * width), 2 * width)
            total = acc[b] + jnp.dot(a, wgu[w, :], preferred_element_type=f32)
            hid[b] = act(total[:, :ff], total[:, ff:])

    for load in loads:
        load.wait()

    def several(c, blocks):
        def step(i, carry):
            b = blocks[-1]
            for n in range(len(blocks) - 2, -1, -1):
                b = jnp.where(i == n, blocks[n], b)
            up(c, b)
            return carry

        lax.fori_loop(0, len(blocks), step, 0)

    def dispatch(i, carry):
        @pl.when(i < nc)
        def _():
            c = i
            all_got(recv, a_r, c)
            packed = jnp.dot(p_ref[...], recv[c], preferred_element_type=f32).astype(bf16)
            gath[c, d] = packed
            for j in (0, 1, 2):
                gcopy(c, j).start()
            lg_ref[...] += lax.dot_general(
                packed, rw_ref[:, lanes(c)], (((1,), (1,)), ((), ())), preferred_element_type=f32
            )

        @pl.when((i >= 1) & (i < nc + 1))
        def _():
            c = i - 1
            gcopy(c, 0).wait_recv()
            gcopy(c, 3).start()
            gcopy(c, 1).wait_recv()
            gcopy(c, 4).start()
            gcopy(c, 5).start()
            gcopy(c, 6).start()
            gcopy(c, 2).wait_recv()
            several(c, (d, dl, dr, dq))

        @pl.when((i >= 2) & (i < nc + 2))
        def _():
            c = i - 2
            gcopy(c, 3).wait_recv()
            gcopy(c, 4).wait_recv()
            gcopy(c, 7).start()
            gcopy(c, 5).wait_recv()
            gcopy(c, 6).wait_recv()
            several(c, (do, xl * 2 + (1 - core), xr * 2 + (1 - core)))
            gcopy(c, 7).wait_recv()
            several(c, (xo * 2 + (1 - core),))

        return carry

    lax.fori_loop(0, nc + 2, dispatch, 0)

    def drain(c, carry):
        for j in range(8):
            gcopy(c, j).wait_send()
        all_sent(outg, a_s, c)
        return carry

    lax.fori_loop(0, nc, drain, 0)

    own_logit = jnp.where(iota((ROOM, experts), 1) == e, lg_ref[...], 0.0)
    gate = jax.nn.sigmoid(jnp.sum(own_logit, axis=1, keepdims=True))
    gt_ref[...] = jnp.broadcast_to(gate, gt_ref.shape)

    def mine(c, k):
        return acc.at[k + 4 * (c % 2), :, pl.ds(pl.multiple_of((c // 2) * width, width), width)]

    def rcopy(c, j):
        src, dst, to = [
            (gath.at[c, 0], prec.at[c, 0], partner),
            (gath.at[c, 1], prec.at[c, 1], partner),
            (gath.at[c, 2], prec.at[c, 2], partner),
            (gath.at[c, 3], prec.at[c, 3], partner),
            (gath.at[c, 4, lo], hrec.at[c, lo], right),
            (gath.at[c, 4, hi], hrec.at[c, hi], left),
            (gath.at[c, 5], srec.at[c, 0], right),
            (gath.at[c, 6], srec.at[c, 1], left),
        ][j]
        return remote(
            src_ref=src, dst_ref=dst, send_sem=r_s.at[c, j], recv_sem=r_r.at[c, j], device_id=to
        )

    def down(c, b):
        return jnp.dot(hid[b], wdn[:, lanes(c)], preferred_element_type=jnp.float32)

    def pair(c, k, n):
        return mine(c, k)[...] + prec[c, n].astype(jnp.float32)

    def combine(i, carry):
        @pl.when((i >= 1) & (i < nc + 1))
        def _():
            c = i - 1
            rcopy(c, 0).wait_recv()
            gath[c, 4] = pair(c, xo, 0).astype(jnp.bfloat16)
            rcopy(c, 4).start()
            rcopy(c, 5).start()

        @pl.when((i >= 2) & (i < nc + 2))
        def _():
            c = i - 2
            rcopy(c, 1).wait_recv()
            rcopy(c, 2).wait_recv()
            to_right, to_left = pair(c, xr, 1), pair(c, xl, 2)
            rcopy(c, 4).wait_recv()
            gath[c, 5, lo] = (to_right[:HALF] + hrec[c, lo].astype(jnp.float32)).astype(jnp.bfloat16)
            gath[c, 5, hi] = to_right[HALF:].astype(jnp.bfloat16)
            rcopy(c, 6).start()
            rcopy(c, 5).wait_recv()
            gath[c, 6, lo] = to_left[:HALF].astype(jnp.bfloat16)
            gath[c, 6, hi] = (to_left[HALF:] + hrec[c, hi].astype(jnp.float32)).astype(jnp.bfloat16)
            rcopy(c, 7).start()

        @pl.when(i < nc)
        def _():
            c = i

            for k in range(4):
                k_x = (xo, xr, xl, x)[k]
                gath[c, k] = down(c, k_x * 2 + (1 - core)).astype(jnp.bfloat16)
                rcopy(c, k).start()

            def keep(k, carry):
                mine(c, k)[...] = down(c, k * 2 + core)
                return carry

            lax.fori_loop(0, 4, keep, 0)

        @pl.when(i >= 3)
        def _():
            c = i - 3
            rcopy(c, 3).wait_recv()
            total = pair(c, x, 3)
            rcopy(c, 6).wait_recv()
            rcopy(c, 7).wait_recv()
            total = total + srec[c, 0].astype(jnp.float32) + srec[c, 1].astype(jnp.float32)
            total = total * gt_ref[...]
            outg[c] = jnp.dot(
                q_ref[...], total.astype(jnp.bfloat16), preferred_element_type=jnp.float32
            ).astype(jnp.bfloat16)
            scatter(outg, arr, b_s, b_r)(c, 0)

        return carry

    lax.fori_loop(0, nc + 3, combine, 0)

    def finish(c, carry):
        all_got(arr, b_r, c)
        got = arr[c]
        o_ref[:, lanes(c)] = jnp.dot(m_ref[...], got, preferred_element_type=f32).astype(bf16)
        return carry

    lax.fori_loop(0, nc, finish, 0)

    def drain_back(c, carry):
        for j in range(8):
            rcopy(c, j).wait_send()
        all_sent(outg, b_s, c)
        return carry

    lax.fori_loop(0, nc, drain_back, 0)


def per_device(tokens, norm_gain, router_weight, w_gate, w_up, w_down, selected):
    n_dp = lax.axis_size("dp")
    n_expert = lax.axis_size("expert")
    tok_rows, model_width = tokens.shape
    experts, capacity = selected.shape
    ff = w_gate.shape[2]
    width = model_width // CHUNKS
    rows = n_expert * SLOT
    vmem = pl.BlockSpec(memory_space=pltpu.VMEM)
    hbm = pl.BlockSpec(memory_space=pl.ANY)
    bf16, f32 = jnp.bfloat16, jnp.float32
    dma = pltpu.SemaphoreType.DMA
    return pl.pallas_call(
        functools.partial(moe_kernel, n_expert),
        out_shape=jax.ShapeDtypeStruct((tok_rows, model_width), bf16),
        in_specs=[vmem] * 4 + [hbm] * 3,
        out_specs=vmem,
        scratch_shapes=[
            pltpu.VMEM((CHUNKS, rows, width), bf16),
            pltpu.VMEM((CHUNKS, rows, width), bf16),
            pltpu.VMEM((CHUNKS, n_dp, ROOM, width), bf16),
            pltpu.VMEM((n_dp, ROOM, 2 * ff), f32),
            pltpu.VMEM((n_dp, ROOM, ff), bf16),
            pltpu.VMEM((model_width, 2 * ff), bf16),
            pltpu.VMEM((ff, model_width), bf16),
            pltpu.VMEM((CHUNKS, n_dp // 2, ROOM, width), bf16),
            pltpu.VMEM((CHUNKS, ROOM, width), bf16),
            pltpu.VMEM((CHUNKS, 2, ROOM, width), bf16),
            pltpu.VMEM((CHUNKS, rows, width), bf16),
            pltpu.VMEM((rows, tok_rows), bf16),
            pltpu.VMEM((tok_rows, model_width), bf16),
            pltpu.VMEM((ROOM, rows), bf16),
            pltpu.VMEM((rows, ROOM), bf16),
            pltpu.VMEM((tok_rows, rows), bf16),
            pltpu.VMEM((ROOM, experts), f32),
            pltpu.VMEM((ROOM, width), f32),
            dma((3,)),
            dma((CHUNKS,)),
            dma((CHUNKS,)),
            dma((CHUNKS, 8)),
            dma((CHUNKS, 8)),
            dma((CHUNKS, 8)),
            dma((CHUNKS, 8)),
            dma((CHUNKS,)),
            dma((CHUNKS,)),
        ],
        compiler_params=pltpu.CompilerParams(
            collective_id=0, has_side_effects=True, vmem_limit_bytes=67043328
        ),
    )(
        tokens,
        norm_gain,
        router_weight.T,
        selected,
        w_gate.reshape(model_width, ff),
        w_up.reshape(model_width, ff),
        w_down.reshape(ff, model_width),
    )


def solution(mesh):
    in_specs = (
        P(("dp", "expert"), None),
        P(),
        P(),
        P("expert", None, "dp"),
        P("expert", None, "dp"),
        P("expert", "dp", None),
        P(),
    )
    out_specs = P(("dp", "expert"), None)
    return jax.shard_map(
        per_device, mesh=mesh, in_specs=in_specs, out_specs=out_specs, check_vma=False
    )
```

```python
import functools

import jax
import jax.numpy as jnp
from jax import lax
from jax.experimental import pallas as pl
from jax.experimental.pallas import tpu as pltpu
from jax.sharding import PartitionSpec as P

SLOT = 16
ROOM = 336
HALF = 176
CHUNKS = 8


def copy_pairs(mesh_id):
    return functools.partial(pltpu.make_async_remote_copy, device_id_type=mesh_id)


def moe_kernel(
    n_expert,
    tok_ref,
    gain_ref,
    rw_ref,
    sel_ref,
    wg_ref,
    wu_ref,
    wd_ref,
    o_ref,
    outg,
    recv,
    gath,
    acc,
    hid,
    wgu,
    wdn,
    prec,
    hrec,
    srec,
    arr,
    s_ref,
    n_ref,
    p_ref,
    q_ref,
    m_ref,
    lg_ref,
    gt_ref,
    wsem,
    a_s,
    a_r,
    g_s,
    g_r,
    r_s,
    r_r,
    b_s,
    b_r,
):
    nc = CHUNKS
    width = outg.shape[2]
    ff = hid.shape[2]
    rows = n_expert * SLOT
    remote = copy_pairs(pl.DeviceIdType.MESH)
    d = lax.axis_index("dp")
    e = lax.axis_index("expert")
    x, core = d // 2, d % 2
    xr, xl, xo = (x + 1) % 4, (x + 3) % 4, (x + 2) % 4
    dl, dr, do, dq = xl * 2 + core, xr * 2 + core, xo * 2 + core, x * 2 + (1 - core)
    right, left, partner = (dr, e), (dl, e), (dq, e)

    def peer(k):
        return (d, (e + k) % n_expert)

    barrier = pltpu.get_barrier_semaphore()

    def greet(k, carry):
        pl.semaphore_signal(barrier, inc=1, device_id=peer(k), device_id_type=pl.DeviceIdType.MESH)
        return carry

    lax.fori_loop(1, n_expert, greet, 0)
    for who in (right, left, partner):
        pl.semaphore_signal(barrier, inc=1, device_id=who, device_id_type=pl.DeviceIdType.MESH)

    def lanes(c):
        return pl.ds(pl.multiple_of(c * width, width), width)

    loads = [
        pltpu.make_async_copy(wg_ref, wgu.at[:, pl.ds(0, ff)], wsem.at[0]),
        pltpu.make_async_copy(wu_ref, wgu.at[:, pl.ds(ff, ff)], wsem.at[1]),
        pltpu.make_async_copy(wd_ref, wdn, wsem.at[2]),
    ]
    for load in loads:
        load.start()

    f32, bf16 = jnp.float32, jnp.bfloat16
    tok_rows = tok_ref.shape[0]
    experts, capacity = sel_ref.shape

    def iota(shape, axis):
        return lax.broadcasted_iota(jnp.int32, shape, axis)

    def one_hot(mask):
        return jnp.where(mask, 1.0, 0.0).astype(bf16)

    def flip(a):
        n = a.shape[1]
        eye = one_hot(iota((n, n), 0) == iota((n, n), 1))
        turned = lax.dot_general(eye, a, (((1,), (1,)), ((), ())), preferred_element_type=f32)
        return turned.astype(bf16)

    tok = tok_ref[...].astype(f32)
    mean_square = jnp.mean(tok * tok, axis=1, keepdims=True)
    n_ref[...] = (tok * lax.rsqrt(mean_square + 1e-06) * gain_ref[...].astype(f32)[None, :]).astype(bf16)

    lowest = (d * n_expert + e) * tok_rows
    sel = sel_ref[...]
    below = jnp.sum(jnp.where(sel < lowest, 1.0, 0.0), axis=1, keepdims=True)
    rank = iota((experts, capacity), 1).astype(f32) - below
    inside = (sel >= lowest) & (sel < lowest + tok_rows)
    local = jnp.where(inside, sel - lowest + 1, 0).astype(f32)
    token = iota((experts, tok_rows), 1).astype(f32) + 1.0
    by_slot = []
    for k in range(SLOT):
        found = jnp.sum(jnp.where(rank == float(k), local, 0.0), axis=1, keepdims=True)
        by_slot.append(jnp.where(found == token, 1.0, 0.0))
    by_slot = jnp.concatenate(by_slot, axis=0).astype(bf16)
    r = iota((rows, rows), 0)
    order = one_hot(iota((rows, rows), 1) == (r & (SLOT - 1)) * experts + lax.shift_right_logical(r, 4))
    s_ref[...] = jnp.dot(order, by_slot, preferred_element_type=f32).astype(bf16)
    pl.semaphore_wait(barrier, n_expert - 1 + 3)

    def slot(k):
        return pl.ds(pl.multiple_of(k * SLOT, SLOT), SLOT)

    def scatter(src, dst, send, got):
        def chunk(c, carry):
            def one(k, carry):
                to = (e + k) % n_expert
                remote(
                    src_ref=src.at[c, slot(to)],
                    dst_ref=dst.at[c, slot(e)],
                    send_sem=send.at[c],
                    recv_sem=got.at[c],
                    device_id=(d, to),
                ).start()
                return carry

            lax.fori_loop(1, n_expert, one, 0)
            pltpu.make_async_copy(src.at[c, slot(e)], dst.at[c, slot(e)], got.at[c]).start()
            return carry

        return chunk

    def all_got(dst, got, c):
        pltpu.make_async_copy(dst.at[c], dst.at[c], got.at[c]).wait()

    def all_sent(src, send, c):
        part = src.at[c, pl.ds(0, rows - SLOT)]
        pltpu.make_async_copy(part, part, send.at[c]).wait()

    def fill(c, carry):
        outg[c] = jnp.dot(s_ref[...], n_ref[:, lanes(c)], preferred_element_type=f32).astype(bf16)
        return scatter(outg, recv, a_s, a_r)(c, carry)

    lax.fori_loop(0, nc, fill, 0)

    row = sel_ref[pl.ds(e, 1), :]
    slot_row = iota((rows, 1), 0)
    lower = (d * n_expert + lax.shift_right_logical(slot_row, 4)) * tok_rows
    rank_in = (slot_row & (SLOT - 1)).astype(f32)
    first = jnp.sum(jnp.where(row < lower, 1.0, 0.0), axis=1, keepdims=True)
    last = jnp.sum(jnp.where(row < lower + tok_rows, 1.0, 0.0), axis=1, keepdims=True)
    start = jnp.sum(jnp.where(row < d * (n_expert * tok_rows), 1.0, 0.0), axis=1, keepdims=True)
    place = jnp.where(rank_in < last - first, first - start + rank_in, -1.0)
    q_ref[...] = one_hot(place == iota((rows, ROOM), 1).astype(f32))
    p_ref[...] = flip(q_ref[...])
    m_ref[...] = flip(s_ref[...])
    acc[...] = jnp.zeros_like(acc)
    lg_ref[...] = jnp.zeros_like(lg_ref)

    lo, hi = pl.ds(0, HALF), pl.ds(HALF, ROOM - HALF)

    def gcopy(c, j):
        block, to = [
            (gath.at[c, d], right),
            (gath.at[c, d], left),
            (gath.at[c, d], partner),
            (gath.at[c, dl, lo], right),
            (gath.at[c, dr, hi], left),
            (gath.at[c, dl], partner),
            (gath.at[c, dr], partner),
            (gath.at[c, do], partner),
        ][j]
        return remote(
            src_ref=block,
            dst_ref=block,
            send_sem=g_s.at[c, j],
            recv_sem=g_r.at[c, j],
            device_id=to,
        )

    def act(v, u):
        g = 0.5 * v * (1.0 + jnp.tanh(0.7978845608028654 * (v + 0.044715 * (v * v * v))))
        return (g * u).astype(bf16)

    def up(c, b):
        @pl.when((c % 2 == 1) & (c < nc - 2))
        def _():
            a = jnp.concatenate([gath[c - 1, b], gath[c, b]], axis=1)
            w = pl.ds(pl.multiple_of((c - 1) * width, 2 * width), 2 * width)
            acc[b] += jnp.dot(a, wgu[w, :], preferred_element_type=f32)

        @pl.when(c == nc - 2)
        def _():
            w = pl.ds((nc - 2) * width, width)
            acc[b] += jnp.dot(gath[c, b], wgu[w, :], preferred_element_type=f32)

        @pl.when(c == nc - 1)
        def _():
            w = pl.ds((nc - 1) * width, width)
            total = acc[b] + jnp.dot(gath[c, b], wgu[w, :], preferred_element_type=f32)
            hid[b] = act(total[:, :ff], total[:, ff:])

    for load in loads:
        load.wait()

    def several(c, blocks):
        def step(i, carry):
            b = blocks[-1]
            for n in range(len(blocks) - 2, -1, -1):
                b = jnp.where(i == n, blocks[n], b)
            up(c, b)
            return carry

        lax.fori_loop(0, len(blocks), step, 0)

    def dispatch(i, carry):
        @pl.when(i < nc)
        def _():
            c = i
            all_got(recv, a_r, c)
            packed = jnp.dot(p_ref[...], recv[c], preferred_element_type=f32).astype(bf16)
            gath[c, d] = packed
            for j in (0, 1, 2):
                gcopy(c, j).start()
            lg_ref[...] += lax.dot_general(
                packed, rw_ref[:, lanes(c)], (((1,), (1,)), ((), ())), preferred_element_type=f32
            )

        @pl.when((i >= 1) & (i < nc + 1))
        def _():
            c = i - 1
            gcopy(c, 0).wait_recv()
            gcopy(c, 3).start()
            gcopy(c, 1).wait_recv()
            gcopy(c, 4).start()
            gcopy(c, 5).start()
            gcopy(c, 6).start()
            gcopy(c, 2).wait_recv()
            several(c, (d, dl, dr, dq))

        @pl.when((i >= 2) & (i < nc + 2))
        def _():
            c = i - 2
            gcopy(c, 3).wait_recv()
            gcopy(c, 4).wait_recv()
            gcopy(c, 7).start()
            gcopy(c, 5).wait_recv()
            gcopy(c, 6).wait_recv()
            several(c, (do, xl * 2 + (1 - core), xr * 2 + (1 - core)))
            gcopy(c, 7).wait_recv()
            several(c, (xo * 2 + (1 - core),))

        return carry

    lax.fori_loop(0, nc + 2, dispatch, 0)

    def drain(c, carry):
        for j in range(8):
            gcopy(c, j).wait_send()
        all_sent(outg, a_s, c)
        return carry

    lax.fori_loop(0, nc, drain, 0)

    own_logit = jnp.where(iota((ROOM, experts), 1) == e, lg_ref[...], 0.0)
    gate = jax.nn.sigmoid(jnp.sum(own_logit, axis=1, keepdims=True))
    gt_ref[...] = jnp.broadcast_to(gate, gt_ref.shape)

    def mine(c, k):
        return acc.at[k + 4 * (c % 2), :, pl.ds(pl.multiple_of((c // 2) * width, width), width)]

    def rcopy(c, j):
        src, dst, to = [
            (gath.at[c, 0], prec.at[c, 0], partner),
            (gath.at[c, 1], prec.at[c, 1], partner),
            (gath.at[c, 2], prec.at[c, 2], partner),
            (gath.at[c, 3], prec.at[c, 3], partner),
            (gath.at[c, 4, lo], hrec.at[c, lo], right),
            (gath.at[c, 4, hi], hrec.at[c, hi], left),
            (gath.at[c, 5], srec.at[c, 0], right),
            (gath.at[c, 6], srec.at[c, 1], left),
        ][j]
        return remote(
            src_ref=src, dst_ref=dst, send_sem=r_s.at[c, j], recv_sem=r_r.at[c, j], device_id=to
        )

    def down(c, b):
        return jnp.dot(hid[b], wdn[:, lanes(c)], preferred_element_type=jnp.float32)

    def pair(c, k, n):
        return mine(c, k)[...] + prec[c, n].astype(jnp.float32)

    def combine(i, carry):
        @pl.when((i >= 1) & (i < nc + 1))
        def _():
            c = i - 1
            rcopy(c, 0).wait_recv()
            gath[c, 4] = pair(c, xo, 0).astype(jnp.bfloat16)
            rcopy(c, 4).start()
            rcopy(c, 5).start()

        @pl.when((i >= 2) & (i < nc + 2))
        def _():
            c = i - 2
            rcopy(c, 1).wait_recv()
            rcopy(c, 2).wait_recv()
            to_right, to_left = pair(c, xr, 1), pair(c, xl, 2)
            rcopy(c, 4).wait_recv()
            gath[c, 5, lo] = (to_right[:HALF] + hrec[c, lo].astype(jnp.float32)).astype(jnp.bfloat16)
            gath[c, 5, hi] = to_right[HALF:].astype(jnp.bfloat16)
            rcopy(c, 6).start()
            rcopy(c, 5).wait_recv()
            gath[c, 6, lo] = to_left[:HALF].astype(jnp.bfloat16)
            gath[c, 6, hi] = (to_left[HALF:] + hrec[c, hi].astype(jnp.float32)).astype(jnp.bfloat16)
            rcopy(c, 7).start()

        @pl.when(i >= 3)
        def _():
            c = i - 3
            rcopy(c, 3).wait_recv()
            total = pair(c, x, 3)
            rcopy(c, 6).wait_recv()
            rcopy(c, 7).wait_recv()
            total = total + srec[c, 0].astype(jnp.float32) + srec[c, 1].astype(jnp.float32)
            total = total * gt_ref[...]
            outg[c] = jnp.dot(
                q_ref[...], total.astype(jnp.bfloat16), preferred_element_type=jnp.float32
            ).astype(jnp.bfloat16)
            scatter(outg, arr, b_s, b_r)(c, 0)

        @pl.when(i < nc)
        def _():
            c = i

            for k in range(4):
                k_x = (xo, xr, xl, x)[k]
                gath[c, k] = down(c, k_x * 2 + (1 - core)).astype(jnp.bfloat16)
                rcopy(c, k).start()

            def keep(k, carry):
                mine(c, k)[...] = down(c, k * 2 + core)
                return carry

            lax.fori_loop(0, 4, keep, 0)

        return carry

    lax.fori_loop(0, nc + 3, combine, 0)

    def finish(c, carry):
        all_got(arr, b_r, c)
        got = arr[c]
        o_ref[:, lanes(c)] = jnp.dot(m_ref[...], got, preferred_element_type=f32).astype(bf16)
        return carry

    lax.fori_loop(0, nc, finish, 0)

    def drain_back(c, carry):
        for j in range(8):
            rcopy(c, j).wait_send()
        all_sent(outg, b_s, c)
        return carry

    lax.fori_loop(0, nc, drain_back, 0)


def per_device(tokens, norm_gain, router_weight, w_gate, w_up, w_down, selected):
    n_dp = lax.axis_size("dp")
    n_expert = lax.axis_size("expert")
    tok_rows, model_width = tokens.shape
    experts, capacity = selected.shape
    ff = w_gate.shape[2]
    width = model_width // CHUNKS
    rows = n_expert * SLOT
    vmem = pl.BlockSpec(memory_space=pltpu.VMEM)
    hbm = pl.BlockSpec(memory_space=pl.ANY)
    bf16, f32 = jnp.bfloat16, jnp.float32
    dma = pltpu.SemaphoreType.DMA
    return pl.pallas_call(
        functools.partial(moe_kernel, n_expert),
        out_shape=jax.ShapeDtypeStruct((tok_rows, model_width), bf16),
        in_specs=[vmem] * 4 + [hbm] * 3,
        out_specs=vmem,
        scratch_shapes=[
            pltpu.VMEM((CHUNKS, rows, width), bf16),
            pltpu.VMEM((CHUNKS, rows, width), bf16),
            pltpu.VMEM((CHUNKS, n_dp, ROOM, width), bf16),
            pltpu.VMEM((n_dp, ROOM, 2 * ff), f32),
            pltpu.VMEM((n_dp, ROOM, ff), bf16),
            pltpu.VMEM((model_width, 2 * ff), bf16),
            pltpu.VMEM((ff, model_width), bf16),
            pltpu.VMEM((CHUNKS, n_dp // 2, ROOM, width), bf16),
            pltpu.VMEM((CHUNKS, ROOM, width), bf16),
            pltpu.VMEM((CHUNKS, 2, ROOM, width), bf16),
            pltpu.VMEM((CHUNKS, rows, width), bf16),
            pltpu.VMEM((rows, tok_rows), bf16),
            pltpu.VMEM((tok_rows, model_width), bf16),
            pltpu.VMEM((ROOM, rows), bf16),
            pltpu.VMEM((rows, ROOM), bf16),
            pltpu.VMEM((tok_rows, rows), bf16),
            pltpu.VMEM((ROOM, experts), f32),
            pltpu.VMEM((ROOM, width), f32),
            dma((3,)),
            dma((CHUNKS,)),
            dma((CHUNKS,)),
            dma((CHUNKS, 8)),
            dma((CHUNKS, 8)),
            dma((CHUNKS, 8)),
            dma((CHUNKS, 8)),
            dma((CHUNKS,)),
            dma((CHUNKS,)),
        ],
        compiler_params=pltpu.CompilerParams(
            collective_id=0, has_side_effects=True, vmem_limit_bytes=67043328
        ),
    )(
        tokens,
        norm_gain,
        router_weight.T,
        selected,
        w_gate.reshape(model_width, ff),
        w_up.reshape(model_width, ff),
        w_down.reshape(ff, model_width),
    )


def solution(mesh):
    in_specs = (
        P(("dp", "expert"), None),
        P(),
        P(),
        P("expert", None, "dp"),
        P("expert", None, "dp"),
        P("expert", "dp", None),
        P(),
    )
    out_specs = P(("dp", "expert"), None)
    return jax.shard_map(
        per_device, mesh=mesh, in_specs=in_specs, out_specs=out_specs, check_vma=False
    )
```
